32 devices in a mesh: gx: 4 (over z), gy: 4 (over x, core), gz: 2 (over y).
Axes of the slice: x: 2, y: 2, z: 4, core: 2. Of those that a mesh axis runs over, the one named last changes fastest.
Arguments:
- populations: float32 [19, 16, 32, 512], P(None, 'gz', 'gx', 'gy'), may hold values from 0 to 1, as said below
- omega: float32 [16, 32, 512], P('gz', 'gx', 'gy'), may hold values from 0.8 to 1.7
- obstacle: int32 [16, 32, 512], P('gz', 'gx', 'gy'), may hold values 0 or 1
Outputs:
- lifted: float32 [19, 16, 32, 512], P(None, 'gz', 'gx', 'gy')
- diagnostics: float32 [5], replicated
The draws below stay inside these ranges and needn't reach their ends.
Inputs may be any that keep to these rules, and one draw needn't show every extreme that they name: `populations`: every population lies between 0.3 and 1.7 times its lattice weight.
All inputs are finite; a program needn't handle non-finite values. No bound on the sum of `obstacle` on one device may be relied on, other than what follows from the above.
Results may differ from the reference program's by a relative error of at most 0.0001.
Values sent between devices are 32-bit elements; how exact they have to be, the bound alone decides.
A program may use at most 128 MiB of HBM per device.

```python
import jax
import jax.numpy as jnp

STEPS = 4
JUMP = 2
NX = 32
NY = 512
NZ = 16


def draw_populations(key, part):
    lattice_weights = jnp.array([1.0 / 3.0] + [1.0 / 18.0] * 6 + [1.0 / 36.0] * 12, jnp.float32)[:, None, None, None]
    phases = jax.random.uniform(jax.random.fold_in(key, 7), (3,), jnp.float32, 0.0, 2.0 * jnp.pi)
    zpos = jnp.arange(NZ, dtype=jnp.float32)[None, :, None, None] / NZ
    xpos = jnp.arange(NX, dtype=jnp.float32)[None, None, :, None] / NX
    spread = 0.425 + 0.15 * jnp.sin(2.0 * jnp.pi * zpos + phases[0]) + 0.125 * jnp.sin(2.0 * jnp.pi * xpos + phases[1])
    noise = jax.random.uniform(key, (19, NZ, NX, NY), jnp.float32, -1.0, 1.0)
    return (lattice_weights * (1.0 + spread * noise)).astype(jnp.float32)


def set_ends(drawn, rng, low, high):
    extent = drawn.shape
    index_at = [jax.random.randint(jax.random.fold_in(rng, axis), (), 0, extent[axis]) for axis in range(len(extent))]
    drawn = drawn.at[tuple(index_at)].set(low)
    longest = extent.index(max(extent))
    index_at[longest] = (index_at[longest] + 1) % extent[longest]
    return drawn.at[tuple(index_at)].set(high)


def steps_of(own_key, shape, cuts, least, top_value):
    loudness, own = 1.0, jax.random.fold_in(own_key, 6)
    for dim, parts in cuts:
        heights = jnp.exp(jax.random.uniform(jax.random.fold_in(own, dim), (parts,), jnp.float32, least / len(cuts), top_value / len(cuts)))
        loudness = loudness * jnp.repeat(heights, shape[dim] // parts).reshape([-1 if axis == dim else 1 for axis in range(len(shape))])
    return loudness


def setup_inputs(seed: int = 0) -> dict:
    key_of = jax.random.split(jax.random.key(seed), 4)
    populations = draw_populations(jax.random.fold_in(key_of[3], 71), 0)
    omega = jnp.clip(0.8 + 0.90000004 * jax.random.uniform(key_of[1], (NZ, NX, NY), jnp.float32) ** steps_of(key_of[1], (NZ, NX, NY), ((0, 2), (1, 4), (2, 4)), -0.2, 0.2), 0.8, 1.7)
    obstacle = set_ends((jax.random.randint(key_of[2], (NZ, NX, NY), 0, 8) < 1).astype(jnp.int32), jax.random.fold_in(key_of[2], 1), 0, 1)
    return {"populations": populations, "omega": omega, "obstacle": obstacle}


lattice = [(0, 0, 0), (1, 0, 0), (-1, 0, 0), (0, 1, 0), (0, -1, 0), (0, 0, 1), (0, 0, -1),
           (1, 1, 0), (-1, -1, 0), (1, -1, 0), (-1, 1, 0), (1, 0, 1), (-1, 0, -1), (1, 0, -1), (-1, 0, 1),
           (0, 1, 1), (0, -1, -1), (0, 1, -1), (0, -1, 1)]
weights = [1.0 / 3.0] + [1.0 / 18.0] * 6 + [1.0 / 36.0] * 12
opposite = [0, 2, 1, 4, 3, 6, 5, 8, 7, 10, 9, 12, 11, 14, 13, 16, 15, 18, 17]
limiter = 25.0


def moments(f):
    rho = jnp.sum(f, axis=0)
    comps = []
    for axis_pick in range(3):
        total = jnp.zeros_like(rho)
        for index in range(19):
            comp = lattice[index][axis_pick]
            if comp != 0:
                total = total + comp * f[index]
        comps.append(total)
    return rho, comps[0], comps[1], comps[2]


def equilibrium(rho, momx, momy, momz):
    safe = jnp.maximum(rho, 0.5)
    velx, vely, velz = momx / safe, momy / safe, momz / safe
    square = velx * velx + vely * vely + velz * velz
    rows = []
    for index in range(19):
        cx, cy, cz = lattice[index]
        proj = cx * velx + cy * vely + cz * velz
        rows.append(weights[index] * rho * (1.0 + 3.0 * proj + 4.5 * proj * proj - 1.5 * square))
    return jnp.stack(rows, 0)


def collide(f, omega, solid):
    rho, momx, momy, momz = moments(f)
    feq = equilibrium(rho, momx, momy, momz)
    post = f + omega[None] * (feq - f)
    flipped = jnp.stack([f[opposite[index]] for index in range(19)], 0)
    return jnp.where(solid[None], flipped, post)


def reference(populations, omega, obstacle):
    solid = obstacle == 1
    f = populations
    before = f
    for step in range(STEPS):
        post = collide(f, omega, solid)
        f = jnp.stack([jnp.roll(post[index], (lattice[index][2], lattice[index][0], lattice[index][1]), axis=(0, 1, 2)) for index in range(19)], 0)
        if step == STEPS - 2:
            before = f
    rho_a, jxa, jya, jza = moments(before)
    rho_b, jxb, jyb, jzb = moments(f)
    cells = float(NX * NY * NZ)
    diff_rho = rho_b - rho_a
    diff_x = jxb - jxa
    diff_y = jyb - jya
    diff_z = jzb - jza
    change = jnp.sum(diff_rho * diff_rho + diff_x * diff_x + diff_y * diff_y + diff_z * diff_z) / cells
    gain = JUMP / (1.0 + limiter * change)
    rho_p = rho_b + gain * diff_rho
    jxp = jxb + gain * diff_x
    jyp = jyb + gain * diff_y
    jzp = jzb + gain * diff_z
    lifted = equilibrium(rho_p, jxp, jyp, jzp)
    diagnostics = jnp.stack([change, jnp.sum(jxp) / cells, jnp.sum(jyp) / cells, jnp.sum(jzp) / cells,
                             jnp.sum(jxp * jxp + jyp * jyp + jzp * jzp) / cells])
    return lifted, diagnostics.astype(jnp.float32)
```

```python
import functools

import jax
import jax.numpy as jnp
from jax import lax
from jax.experimental import pallas as pl
from jax.experimental.pallas import tpu as pltpu
from jax.sharding import PartitionSpec as P

STEPS = 4
JUMP = 2
LIMITER = 25.0
AXES = ("gx", "gy", "gz")

LATTICE = [
    (0, 0, 0),
    (1, 0, 0), (-1, 0, 0), (0, 1, 0), (0, -1, 0), (0, 0, 1), (0, 0, -1),
    (1, 1, 0), (-1, -1, 0), (1, -1, 0), (-1, 1, 0),
    (1, 0, 1), (-1, 0, -1), (1, 0, -1), (-1, 0, 1),
    (0, 1, 1), (0, -1, -1), (0, 1, -1), (0, -1, 1),
]
WEIGHTS = [1.0 / 3.0] + [1.0 / 18.0] * 6 + [1.0 / 36.0] * 12
CROSS = [[[i for i in range(19) if LATTICE[i][axis] == sign] for sign in (1, -1)] for axis in range(3)]
ORDER = [i for i in range(19) if LATTICE[i][2] == 0] + CROSS[2][0] + CROSS[2][1]
SLOT = {i: ORDER.index(i) for i in range(19)}
INDEX = {v: i for i, v in enumerate(LATTICE)}


def side(c):
    return 0 if c == 1 else 1


def rank_in(axis, i):
    return CROSS[axis][side(LATTICE[i][axis])].index(i)


def moments(f):
    def total(terms):
        terms = list(terms)
        while len(terms) > 1:
            terms = [terms[j] + terms[j + 1] if j + 1 < len(terms) else terms[j] for j in range(0, len(terms), 2)]
        return terms[0]

    comps = []
    for axis in range(3):
        comps.append(total(f[p] - f[p + 1] for p in range(1, 19, 2) if LATTICE[p][axis] == 1)
                     + 0.0)
    for axis in range(3):
        extra = [f[p] - f[p + 1] for p in range(1, 19, 2) if LATTICE[p][axis] == -1]
        if extra:
            comps[axis] = comps[axis] - total(extra)
    return total(f), comps[0], comps[1], comps[2]


def equilibrium_parts(rho, jx, jy, jz):
    inverse = 3.0 / jnp.maximum(rho, 0.5)
    v = (jx * inverse, jy * inverse, jz * inverse)
    base = 1.0 - (v[0] * v[0] + v[1] * v[1] + v[2] * v[2]) * (1.5 / 9.0)
    return v, base


def projected(v, i):
    out = None
    for comp, vel in zip(LATTICE[i], v):
        if comp == 1:
            out = vel if out is None else out + vel
        elif comp == -1:
            out = -vel if out is None else out - vel
    return out


def collide(f, omega, solid):
    rho, jx, jy, jz = moments(f)
    v, base = equilibrium_parts(rho, jx, jy, jz)
    keep = 1.0 - omega
    scale = omega * rho
    scaled = {w: scale * w for w in set(WEIGHTS)}
    post = [None] * 19
    post[0] = jnp.where(solid, f[0], keep * f[0] + scaled[WEIGHTS[0]] * base)
    for i in range(1, 19, 2):
        p = projected(v, i)
        even = base + 0.5 * (p * p)
        w = scaled[WEIGHTS[i]]
        post[i] = jnp.where(solid, f[i + 1], keep * f[i] + w * (even + p))
        post[i + 1] = jnp.where(solid, f[i], keep * f[i + 1] + w * (even - p))
    return post


def kernel(sizes, cells, pop_hbm, omega_hbm, obstacle_hbm, lifted_ref, diag_ref,
           f_in, om, ob, post, xs, ys, es, hx, hy, hz, hxy, hyz, hxz, cs, before, after, gather,
           load_sem, send_sem, recv_sem, gsend_sem, grecv_sem):
    Z, X, Y = om.shape
    nx, ny, nz = (sizes[a] for a in AXES)
    n = nx * ny * nz
    me = tuple(lax.axis_index(a) for a in AXES)

    def device(offset):
        return {a: lax.rem(me[d] + (offset[d] % sizes[a]), sizes[a]) for d, a in enumerate(AXES)}

    loads = []
    for z in range(Z):
        loads.append(pltpu.make_async_copy(pop_hbm.at[:, z], f_in.at[:, z], load_sem.at[z]))
    loads.append(pltpu.make_async_copy(omega_hbm, om, load_sem.at[Z]))
    loads.append(pltpu.make_async_copy(obstacle_hbm, ob, load_sem.at[Z + 1]))
    for copy in loads[::-1]:
        copy.start()

    far = (nx // 2, ny // 2, nz // 2)
    covered = max(max(far), (sum(far) + 1) // 2) <= STEPS
    wrapped = lambda c: (c[0] % nx, c[1] % ny, c[2] % nz)
    everyone = [(k // (ny * nz), k // nz % ny, k % nz) for k in range(1, n)]
    greet = sorted({wrapped(c) for c in LATTICE} - {(0, 0, 0)}) if covered else everyone
    barrier = pltpu.get_barrier_semaphore()
    for offset in greet:
        pl.semaphore_signal(barrier, inc=1, device_id=device(offset), device_id_type=pl.DeviceIdType.MESH)

    lane = lax.broadcasted_iota(jnp.int32, (X, Y), 1)
    row = lax.broadcasted_iota(jnp.int32, (X, Y), 0)
    zrow = lax.broadcasted_iota(jnp.int32, (Z, Y), 0)
    zlane = lax.broadcasted_iota(jnp.int32, (Z, Y), 1)
    zsides = (1,) if nz == 2 else (1, -1)
    zside = lambda c: 0 if nz == 2 else side(c)

    def messages(s):
        out = []
        for c in (1, -1):
            d = side(c)
            out.append(((0, 0, c), post.at[s, pl.ds(9 + 5 * d, 5), Z - 1 if c == 1 else 0], hz.at[s, d]))
            out.append(((c, 0, 0), xs.at[s, d], hx.at[s, d]))
            out.append(((0, c, 0), ys.at[s, d], hy.at[s, d]))
            for b in (1, -1):
                k = rank_in(0, INDEX[(c, b, 0)])
                out.append(((c, b, 0), xs.at[s, d, k], hxy.at[s, d, side(b)]))
            for b in zsides:
                out.append(((0, c, b), ys.at[s, d], hyz.at[s, d, zside(b)]))
                out.append(((c, 0, b), es.at[s, d], hxz.at[s, d, zside(b)]))
        return [
            pltpu.make_async_remote_copy(
                src_ref=src, dst_ref=dst, send_sem=send_sem.at[s, m], recv_sem=recv_sem.at[s, m],
                device_id=device(offset), device_id_type=pl.DeviceIdType.MESH)
            for m, (offset, src, dst) in enumerate(out)
        ]

    def pack(s):
        for d in (0, 1):
            edge = X - 1 if d == 0 else 0
            for k, i in enumerate(CROSS[0][d]):
                xs[s, d, k] = post[s, SLOT[i], :, edge, :]
            up = rank_in(0, INDEX[(1 - 2 * d, 0, 1)])
            down = rank_in(0, INDEX[(1 - 2 * d, 0, -1)])
            first = post[s, SLOT[INDEX[(1 - 2 * d, 0, 1)]], Z - 1, edge:edge + 1, :]
            second = post[s, SLOT[INDEX[(1 - 2 * d, 0, -1)]], 0, edge:edge + 1, :]
            es[s, d] = jnp.where(row == 0, jnp.broadcast_to(first, (X, Y)), jnp.broadcast_to(second, (X, Y)))
        for d in (0, 1):
            edge = Y - 1 if d == 0 else 0
            tile = jnp.zeros((X, Y), jnp.float32)
            for k, i in enumerate(CROSS[1][d]):
                for z in range(Z):
                    m = k * Z + z
                    moved = pltpu.roll(post[s, SLOT[i], z], (m - edge) % Y, 1)
                    tile = jnp.where(lane == m, moved, tile)
            ys[s, d] = tile

    def columns(s):
        for d in (0, 1):
            for k, i in enumerate(CROSS[0][d]):
                cx, cy, cz = LATTICE[i]
                col = hx[s, d, k]
                if cy:
                    edge = 0 if cy == 1 else Y - 1
                    corner = pltpu.roll(hxy[s, d, side(cy)], cy % Y, 1)
                    col = jnp.where(zlane == edge, corner, pltpu.roll(col, cy % Y, 1))
                if cz:
                    edge = 0 if cz == 1 else Z - 1
                    r = 0 if cz == 1 else 1
                    corner = jnp.broadcast_to(hxz[s, d, zside(cz), r:r + 1, :], (Z, Y))
                    col = jnp.where(zrow == edge, corner, pltpu.roll(col, cz % Z, 0))
                cs[s, d, k] = col

    def streamed(s, z):
        out = []
        for i in range(19):
            cx, cy, cz = LATTICE[i]
            zs = z - cz
            inside = 0 <= zs < Z
            tile = post[s, SLOT[i], zs] if inside else hz[s, side(cz), rank_in(2, i)]
            if cy:
                source = hy[s, side(cy)] if inside else hyz[s, side(cy), zside(cz)]
                m = rank_in(1, i) * Z + zs % Z
                edge = 0 if cy == 1 else Y - 1
                tile = jnp.where(lane == edge, pltpu.roll(source, (edge - m) % Y, 1), pltpu.roll(tile, cy % Y, 1))
            if cx:
                edge = 0 if cx == 1 else X - 1
                col = jnp.broadcast_to(cs[s, side(cx), rank_in(0, i), z:z + 1, :], (X, Y))
                tile = jnp.where(row == edge, col, pltpu.roll(tile, cx % X, 0))
            out.append(tile)
        return out

    sent = []
    loads[Z].wait()
    loads[Z + 1].wait()
    for s in range(STEPS):
        if s:
            columns(s - 1)
        for z in range(Z):
            if s == 0:
                loads[z].wait()
                f = [f_in[i, z] for i in range(19)]
            else:
                f = streamed(s - 1, z)
            if s == STEPS - 1:
                for c, value in enumerate(moments(f)):
                    before[c, z] = value
            new = collide(f, om[z], ob[z] == 1)
            for i in range(19):
                post[s, SLOT[i], z] = new[i]
        pack(s)
        if s == 0:
            pl.semaphore_wait(barrier, len(greet))
        copies = messages(s)
        for copy in copies:
            copy.start()
        for copy in copies:
            copy.wait_recv()
        sent += copies

    columns(STEPS - 1)
    sums = [jnp.zeros((X, Y), jnp.float32) for _ in range(10)]
    for z in range(Z):
        b = moments(streamed(STEPS - 1, z))
        diff = []
        for c in range(4):
            after[c, z] = b[c]
            delta = b[c] - before[c, z]
            before[c, z] = delta
            diff.append(delta)
        change_mom = diff[1] * diff[1] + diff[2] * diff[2] + diff[3] * diff[3]
        terms = (diff[0] * diff[0], change_mom, b[1], b[2], b[3], diff[1], diff[2], diff[3],
                 b[1] * b[1] + b[2] * b[2] + b[3] * b[3],
                 b[1] * diff[1] + b[2] * diff[2] + b[3] * diff[3])
        sums = [a + t for a, t in zip(sums, terms)]
    wide = lax.broadcasted_iota(jnp.int32, (1, Y), 1)
    mine = jnp.zeros((1, Y), jnp.float32)
    for k, tile in enumerate(sums):
        whole = jnp.sum(jnp.sum(tile, axis=0, keepdims=True), axis=1, keepdims=True)
        mine = jnp.where(wide == k, whole, mine)
    slot = (me[0] * ny + me[1]) * nz + me[2]
    gather[slot] = mine
    stat = []
    for k, offset in enumerate(everyone):
        stat.append(pltpu.make_async_remote_copy(
            src_ref=gather.at[slot], dst_ref=gather.at[slot], send_sem=gsend_sem.at[k], recv_sem=grecv_sem.at[k],
            device_id=device(offset), device_id_type=pl.DeviceIdType.MESH))
    for copy in stat:
        copy.start()
    for copy in sent:
        copy.wait_send()
    for copy in stat:
        copy.wait_recv()
    total = jnp.sum(gather[...], axis=0)
    pick = lambda k: jnp.sum(jnp.where(wide == k, total, 0.0), axis=1, keepdims=True)
    t = [pick(k) for k in range(10)]
    change = (t[0] + t[1]) / cells
    gain = JUMP / (1.0 + LIMITER * change)
    diag = [change] + [(t[2 + c] + gain * t[5 + c]) / cells for c in range(3)]
    diag.append((t[8] + 2.0 * gain * t[9] + gain * gain * t[1]) / cells)
    for k, value in enumerate(diag):
        diag_ref[k] = value[0, 0]
    spread = jnp.broadcast_to(gain, (X, Y))
    for z in range(Z):
        rho, jx, jy, jz = (after[c, z] + spread * before[c, z] for c in range(4))
        v, base = equilibrium_parts(rho, jx, jy, jz)
        scaled = {w: rho * w for w in set(WEIGHTS)}
        lifted_ref[0, z] = scaled[WEIGHTS[0]] * base
        for i in range(1, 19, 2):
            p = projected(v, i)
            even = base + 0.5 * (p * p)
            lifted_ref[i, z] = scaled[WEIGHTS[i]] * (even + p)
            lifted_ref[i + 1, z] = scaled[WEIGHTS[i]] * (even - p)
    for copy in stat:
        copy.wait_send()


def solution(mesh):
    sizes = {a: mesh.shape[a] for a in AXES}
    n = sizes["gx"] * sizes["gy"] * sizes["gz"]

    def per_device(populations, omega, obstacle):
        Z, X, Y = omega.shape
        S = STEPS
        nzs = 1 if sizes["gz"] == 2 else 2
        count = 10 + 4 * nzs
        f32 = lambda *shape: pltpu.VMEM(shape, jnp.float32)
        return pl.pallas_call(
            functools.partial(kernel, sizes, float(Z * X * Y * n)),
            out_shape=(jax.ShapeDtypeStruct(populations.shape, jnp.float32), jax.ShapeDtypeStruct((5,), jnp.float32)),
            in_specs=[pl.BlockSpec(memory_space=pl.ANY)] * 3,
            out_specs=(pl.BlockSpec(memory_space=pltpu.VMEM), pl.BlockSpec(memory_space=pltpu.SMEM)),
            scratch_shapes=[
                f32(19, Z, X, Y), f32(Z, X, Y), pltpu.VMEM((Z, X, Y), jnp.int32),
                f32(S, 19, Z, X, Y),
                f32(S, 2, 5, Z, Y), f32(S, 2, X, Y), f32(S, 2, X, Y),
                f32(S, 2, 5, Z, Y), f32(S, 2, X, Y), f32(S, 2, 5, X, Y),
                f32(S, 2, 2, Z, Y), f32(S, 2, nzs, X, Y), f32(S, 2, nzs, X, Y),
                f32(S, 2, 5, Z, Y), f32(4, Z, X, Y), f32(4, Z, X, Y), f32(n, 1, Y),
                pltpu.SemaphoreType.DMA((Z + 2,)),
                pltpu.SemaphoreType.DMA((S, count)), pltpu.SemaphoreType.DMA((S, count)),
                pltpu.SemaphoreType.DMA((n,)), pltpu.SemaphoreType.DMA((n,)),
            ],
            compiler_params=pltpu.CompilerParams(collective_id=0, has_side_effects=True),
        )(populations, omega, obstacle)

    spec = P("gz", "gx", "gy")
    return jax.shard_map(
        per_device, mesh=mesh, in_specs=(P(None, *spec), spec, spec),
        out_specs=(P(None, *spec), P()), check_vma=False)
```

```python
import functools

import jax
import jax.numpy as jnp
from jax import lax
from jax.experimental import pallas as pl
from jax.experimental.pallas import tpu as pltpu
from jax.sharding import PartitionSpec as P

STEPS = 4
JUMP = 2
LIMITER = 25.0
AXES = ("gx", "gy", "gz")

LATTICE = [
    (0, 0, 0),
    (1, 0, 0), (-1, 0, 0), (0, 1, 0), (0, -1, 0), (0, 0, 1), (0, 0, -1),
    (1, 1, 0), (-1, -1, 0), (1, -1, 0), (-1, 1, 0),
    (1, 0, 1), (-1, 0, -1), (1, 0, -1), (-1, 0, 1),
    (0, 1, 1), (0, -1, -1), (0, 1, -1), (0, -1, 1),
]
WEIGHTS = [1.0 / 3.0] + [1.0 / 18.0] * 6 + [1.0 / 36.0] * 12
CROSS = [[[i for i in range(19) if LATTICE[i][axis] == sign] for sign in (1, -1)] for axis in range(3)]
ORDER = [i for i in range(19) if LATTICE[i][2] == 0] + CROSS[2][0] + CROSS[2][1]
SLOT = {i: ORDER.index(i) for i in range(19)}
INDEX = {v: i for i, v in enumerate(LATTICE)}


def side(c):
    return 0 if c == 1 else 1


def rank_in(axis, i):
    return CROSS[axis][side(LATTICE[i][axis])].index(i)


def moments(f):
    def total(terms):
        terms = list(terms)
        while len(terms) > 1:
            terms = [terms[j] + terms[j + 1] if j + 1 < len(terms) else terms[j] for j in range(0, len(terms), 2)]
        return terms[0]

    comps = []
    for axis in range(3):
        comps.append(total(f[p] - f[p + 1] for p in range(1, 19, 2) if LATTICE[p][axis] == 1)
                     + 0.0)
    for axis in range(3):
        extra = [f[p] - f[p + 1] for p in range(1, 19, 2) if LATTICE[p][axis] == -1]
        if extra:
            comps[axis] = comps[axis] - total(extra)
    return total(f), comps[0], comps[1], comps[2]


def equilibrium_parts(rho, jx, jy, jz):
    inverse = 3.0 / jnp.maximum(rho, 0.5)
    v = (jx * inverse, jy * inverse, jz * inverse)
    base = 1.0 - (v[0] * v[0] + v[1] * v[1] + v[2] * v[2]) * (1.5 / 9.0)
    return v, base


def projected(v, i):
    out = None
    for comp, vel in zip(LATTICE[i], v):
        if comp == 1:
            out = vel if out is None else out + vel
        elif comp == -1:
            out = -vel if out is None else out - vel
    return out


def collide(f, omega, solid):
    rho, jx, jy, jz = moments(f)
    v, base = equilibrium_parts(rho, jx, jy, jz)
    keep = 1.0 - omega
    scale = omega * rho
    scaled = {w: scale * w for w in set(WEIGHTS)}
    post = [None] * 19
    post[0] = jnp.where(solid, f[0], keep * f[0] + scaled[WEIGHTS[0]] * base)
    for i in range(1, 19, 2):
        p = projected(v, i)
        even = base + 0.5 * (p * p)
        w = scaled[WEIGHTS[i]]
        post[i] = jnp.where(solid, f[i + 1], keep * f[i] + w * (even + p))
        post[i + 1] = jnp.where(solid, f[i], keep * f[i + 1] + w * (even - p))
    return post


def kernel(sizes, pop_hbm, omega_hbm, obstacle_hbm, total_ref, after_hbm, change_hbm,
           f_in, om, ob, post, xs, ys, es, hx, hy, hz, hxy, hyz, hxz, cs, before, after, gather,
           load_sem, out_sem, send_sem, recv_sem, gsend_sem, grecv_sem):
    Z, X, Y = om.shape
    nx, ny, nz = (sizes[a] for a in AXES)
    n = nx * ny * nz
    me = tuple(lax.axis_index(a) for a in AXES)

    def device(offset):
        return {a: lax.rem(me[d] + (offset[d] % sizes[a]), sizes[a]) for d, a in enumerate(AXES)}

    loads = []
    for z in range(Z):
        loads.append(pltpu.make_async_copy(pop_hbm.at[:, z], f_in.at[:, z], load_sem.at[z]))
    loads.append(pltpu.make_async_copy(omega_hbm, om, load_sem.at[Z]))
    loads.append(pltpu.make_async_copy(obstacle_hbm, ob, load_sem.at[Z + 1]))
    for copy in loads[::-1]:
        copy.start()

    far = (nx // 2, ny // 2, nz // 2)
    covered = max(max(far), (sum(far) + 1) // 2) <= STEPS
    wrapped = lambda c: (c[0] % nx, c[1] % ny, c[2] % nz)
    everyone = [(k // (ny * nz), k // nz % ny, k % nz) for k in range(1, n)]
    greet = sorted({wrapped(c) for c in LATTICE} - {(0, 0, 0)}) if covered else everyone
    barrier = pltpu.get_barrier_semaphore()
    for offset in greet:
        pl.semaphore_signal(barrier, inc=1, device_id=device(offset), device_id_type=pl.DeviceIdType.MESH)

    lane = lax.broadcasted_iota(jnp.int32, (X, Y), 1)
    row = lax.broadcasted_iota(jnp.int32, (X, Y), 0)
    zrow = lax.broadcasted_iota(jnp.int32, (Z, Y), 0)
    zlane = lax.broadcasted_iota(jnp.int32, (Z, Y), 1)
    zsides = (1,) if nz == 2 else (1, -1)
    zside = lambda c: 0 if nz == 2 else side(c)

    def messages(s):
        out = []
        for c in (1, -1):
            d = side(c)
            out.append(((0, 0, c), post.at[s, pl.ds(9 + 5 * d, 5), Z - 1 if c == 1 else 0], hz.at[s, d]))
            out.append(((c, 0, 0), xs.at[s, d], hx.at[s, d]))
            out.append(((0, c, 0), ys.at[s, d], hy.at[s, d]))
            for b in (1, -1):
                k = rank_in(0, INDEX[(c, b, 0)])
                out.append(((c, b, 0), xs.at[s, d, k], hxy.at[s, d, side(b)]))
            for b in zsides:
                out.append(((0, c, b), ys.at[s, d], hyz.at[s, d, zside(b)]))
                out.append(((c, 0, b), es.at[s, d], hxz.at[s, d, zside(b)]))
        copies = [
            (offset, pltpu.make_async_remote_copy(
                src_ref=src, dst_ref=dst, send_sem=send_sem.at[s, m], recv_sem=recv_sem.at[s, m],
                device_id=device(offset), device_id_type=pl.DeviceIdType.MESH))
            for m, (offset, src, dst) in enumerate(out)
        ]
        along_x = [c for o, c in copies if o[0]]
        along_z = [c for o, c in copies if not o[0] and not o[1]]
        along_y = [c for o, c in copies if not o[0] and o[1]]
        return along_x, along_z, along_y

    def pack_x(s):
        for d in (0, 1):
            edge = X - 1 if d == 0 else 0
            for k, i in enumerate(CROSS[0][d]):
                xs[s, d, k] = post[s, SLOT[i], :, edge, :]
            up = rank_in(0, INDEX[(1 - 2 * d, 0, 1)])
            down = rank_in(0, INDEX[(1 - 2 * d, 0, -1)])
            first = post[s, SLOT[INDEX[(1 - 2 * d, 0, 1)]], Z - 1, edge:edge + 1, :]
            second = post[s, SLOT[INDEX[(1 - 2 * d, 0, -1)]], 0, edge:edge + 1, :]
            es[s, d] = jnp.where(row == 0, jnp.broadcast_to(first, (X, Y)), jnp.broadcast_to(second, (X, Y)))

    def pack_y(s):
        for d in (0, 1):
            edge = Y - 1 if d == 0 else 0
            tile = jnp.zeros((X, Y), jnp.float32)
            for k, i in enumerate(CROSS[1][d]):
                for z in range(Z):
                    m = k * Z + z
                    moved = pltpu.roll(post[s, SLOT[i], z], (m - edge) % Y, 1)
                    tile = jnp.where(lane == m, moved, tile)
            ys[s, d] = tile

    def columns(s):
        for d in (0, 1):
            for k, i in enumerate(CROSS[0][d]):
                cx, cy, cz = LATTICE[i]
                col = hx[s, d, k]
                if cy:
                    edge = 0 if cy == 1 else Y - 1
                    corner = pltpu.roll(hxy[s, d, side(cy)], cy % Y, 1)
                    col = jnp.where(zlane == edge, corner, pltpu.roll(col, cy % Y, 1))
                if cz:
                    edge = 0 if cz == 1 else Z - 1
                    r = 0 if cz == 1 else 1
                    corner = jnp.broadcast_to(hxz[s, d, zside(cz), r:r + 1, :], (Z, Y))
                    col = jnp.where(zrow == edge, corner, pltpu.roll(col, cz % Z, 0))
                cs[s, d, k] = col

    def streamed(s, z):
        out = []
        for i in range(19):
            cx, cy, cz = LATTICE[i]
            zs = z - cz
            inside = 0 <= zs < Z
            tile = post[s, SLOT[i], zs] if inside else hz[s, side(cz), rank_in(2, i)]
            if cy:
                source = hy[s, side(cy)] if inside else hyz[s, side(cy), zside(cz)]
                m = rank_in(1, i) * Z + zs % Z
                edge = 0 if cy == 1 else Y - 1
                tile = jnp.where(lane == edge, pltpu.roll(source, (edge - m) % Y, 1), pltpu.roll(tile, cy % Y, 1))
            if cx:
                edge = 0 if cx == 1 else X - 1
                col = jnp.broadcast_to(cs[s, side(cx), rank_in(0, i), z:z + 1, :], (X, Y))
                tile = jnp.where(row == edge, col, pltpu.roll(tile, cx % X, 0))
            out.append(tile)
        return out

    sent = []
    loads[Z].wait()
    loads[Z + 1].wait()
    for s in range(STEPS):
        if s:
            columns(s - 1)
        for z in range(Z):
            if s == 0:
                loads[z].wait()
                f = [f_in[i, z] for i in range(19)]
            else:
                f = streamed(s - 1, z)
            if s == STEPS - 1:
                for c, value in enumerate(moments(f)):
                    before[c, z] = value
            new = collide(f, om[z], ob[z] == 1)
            for i in range(19):
                post[s, SLOT[i], z] = new[i]
        along_x, along_z, along_y = messages(s)
        pack_x(s)
        if s == 0:
            pl.semaphore_wait(barrier, len(greet))
        for copy in along_x + along_z:
            copy.start()
        pack_y(s)
        for copy in along_y:
            copy.start()
        copies = along_y + along_z + along_x
        for copy in copies:
            copy.wait_recv()
        sent += copies

    columns(STEPS - 1)
    sums = [jnp.zeros((X, Y), jnp.float32) for _ in range(10)]
    for z in range(Z):
        b = moments(streamed(STEPS - 1, z))
        diff = []
        for c in range(4):
            after[c, z] = b[c]
            delta = b[c] - before[c, z]
            before[c, z] = delta
            diff.append(delta)
        change_mom = diff[1] * diff[1] + diff[2] * diff[2] + diff[3] * diff[3]
        terms = (diff[0] * diff[0], change_mom, b[1], b[2], b[3], diff[1], diff[2], diff[3],
                 b[1] * b[1] + b[2] * b[2] + b[3] * b[3],
                 b[1] * diff[1] + b[2] * diff[2] + b[3] * diff[3])
        sums = [a + t for a, t in zip(sums, terms)]
    wide = lax.broadcasted_iota(jnp.int32, (1, Y), 1)
    mine = jnp.zeros((1, Y), jnp.float32)
    for k, tile in enumerate(sums):
        whole = jnp.sum(jnp.sum(tile, axis=0, keepdims=True), axis=1, keepdims=True)
        mine = jnp.where(wide == k, whole, mine)
    slot = (me[0] * ny + me[1]) * nz + me[2]
    gather[slot] = mine
    stat = []
    for k, offset in enumerate(everyone):
        stat.append(pltpu.make_async_remote_copy(
            src_ref=gather.at[slot], dst_ref=gather.at[slot], send_sem=gsend_sem.at[k], recv_sem=grecv_sem.at[k],
            device_id=device(offset), device_id_type=pl.DeviceIdType.MESH))
    for copy in stat:
        copy.start()
    out = [pltpu.make_async_copy(after, after_hbm, out_sem.at[0]),
           pltpu.make_async_copy(before, change_hbm, out_sem.at[1])]
    for copy in out:
        copy.start()
    for copy in sent:
        copy.wait_send()
    for copy in stat:
        copy.wait_recv()
    total_ref[...] = jnp.sum(gather[...], axis=0)
    for copy in stat:
        copy.wait_send()
    for copy in out:
        copy.wait()


def lift_kernel(cells, total_ref, after, before, lifted_ref, diag_ref):
    Z, X, Y = after.shape[1:]
    wide = lax.broadcasted_iota(jnp.int32, (1, Y), 1)
    total = total_ref[...]
    pick = lambda k: jnp.sum(jnp.where(wide == k, total, 0.0), axis=1, keepdims=True)
    t = [pick(k) for k in range(10)]
    change = (t[0] + t[1]) / cells
    gain = JUMP / (1.0 + LIMITER * change)
    diag = [change] + [(t[2 + c] + gain * t[5 + c]) / cells for c in range(3)]
    diag.append((t[8] + 2.0 * gain * t[9] + gain * gain * t[1]) / cells)
    for k, value in enumerate(diag):
        diag_ref[k] = value[0, 0]
    spread = jnp.broadcast_to(gain, (X, Y))
    for z in range(Z):
        rho, jx, jy, jz = (after[c, z] + spread * before[c, z] for c in range(4))
        v, base = equilibrium_parts(rho, jx, jy, jz)
        scaled = {w: rho * w for w in set(WEIGHTS)}
        lifted_ref[0, z] = scaled[WEIGHTS[0]] * base
        for i in range(1, 19, 2):
            p = projected(v, i)
            even = base + 0.5 * (p * p)
            lifted_ref[i, z] = scaled[WEIGHTS[i]] * (even + p)
            lifted_ref[i + 1, z] = scaled[WEIGHTS[i]] * (even - p)


def solution(mesh):
    sizes = {a: mesh.shape[a] for a in AXES}
    n = sizes["gx"] * sizes["gy"] * sizes["gz"]

    def per_device(populations, omega, obstacle):
        Z, X, Y = omega.shape
        S = STEPS
        nzs = 1 if sizes["gz"] == 2 else 2
        count = 10 + 4 * nzs
        f32 = lambda *shape: pltpu.VMEM(shape, jnp.float32)
        shape = lambda *dims: jax.ShapeDtypeStruct(dims, jnp.float32)
        vmem, smem = pl.BlockSpec(memory_space=pltpu.VMEM), pl.BlockSpec(memory_space=pltpu.SMEM)
        any_space = pl.BlockSpec(memory_space=pl.ANY)
        total, after, change = pl.pallas_call(
            functools.partial(kernel, sizes),
            out_shape=(shape(1, Y), shape(4, Z, X, Y), shape(4, Z, X, Y)),
            in_specs=[pl.BlockSpec(memory_space=pl.ANY)] * 3,
            out_specs=(vmem, any_space, any_space),
            scratch_shapes=[
                f32(19, Z, X, Y), f32(Z, X, Y), pltpu.VMEM((Z, X, Y), jnp.int32),
                f32(S, 19, Z, X, Y),
                f32(S, 2, 5, Z, Y), f32(S, 2, X, Y), f32(S, 2, X, Y),
                f32(S, 2, 5, Z, Y), f32(S, 2, X, Y), f32(S, 2, 5, X, Y),
                f32(S, 2, 2, Z, Y), f32(S, 2, nzs, X, Y), f32(S, 2, nzs, X, Y),
                f32(S, 2, 5, Z, Y), f32(4, Z, X, Y), f32(4, Z, X, Y), f32(n, 1, Y),
                pltpu.SemaphoreType.DMA((Z + 2,)), pltpu.SemaphoreType.DMA((2,)),
                pltpu.SemaphoreType.DMA((S, count)), pltpu.SemaphoreType.DMA((S, count)),
                pltpu.SemaphoreType.DMA((n,)), pltpu.SemaphoreType.DMA((n,)),
            ],
            compiler_params=pltpu.CompilerParams(collective_id=0, has_side_effects=True),
        )(populations, omega, obstacle)
        return pl.pallas_call(
            functools.partial(lift_kernel, float(Z * X * Y * n)),
            out_shape=(shape(*populations.shape), shape(5)),
            in_specs=[vmem] * 3,
            out_specs=(vmem, smem),
        )(total, after, change)

    spec = P("gz", "gx", "gy")
    return jax.shard_map(
        per_device, mesh=mesh, in_specs=(P(None, *spec), spec, spec),
        out_specs=(P(None, *spec), P()), check_vma=False)
```

```python
import functools

import jax
import jax.numpy as jnp
from jax import lax
from jax.experimental import pallas as pl
from jax.experimental.pallas import tpu as pltpu
from jax.sharding import PartitionSpec as P

STEPS = 4
JUMP = 2
LIMITER = 25.0
AXES = ("gx", "gy", "gz")

LATTICE = [
    (0, 0, 0),
    (1, 0, 0), (-1, 0, 0), (0, 1, 0), (0, -1, 0), (0, 0, 1), (0, 0, -1),
    (1, 1, 0), (-1, -1, 0), (1, -1, 0), (-1, 1, 0),
    (1, 0, 1), (-1, 0, -1), (1, 0, -1), (-1, 0, 1),
    (0, 1, 1), (0, -1, -1), (0, 1, -1), (0, -1, 1),
]
WEIGHTS = [1.0 / 3.0] + [1.0 / 18.0] * 6 + [1.0 / 36.0] * 12
CROSS = [[[i for i in range(19) if LATTICE[i][axis] == sign] for sign in (1, -1)] for axis in range(3)]
ORDER = [i for i in range(19) if LATTICE[i][2] == 0] + CROSS[2][0] + CROSS[2][1]
SLOT = {i: ORDER.index(i) for i in range(19)}
INDEX = {v: i for i, v in enumerate(LATTICE)}


def side(c):
    return 0 if c == 1 else 1


def rank_in(axis, i):
    return CROSS[axis][side(LATTICE[i][axis])].index(i)


def moments(f):
    def total(terms):
        terms = list(terms)
        while len(terms) > 1:
            terms = [terms[j] + terms[j + 1] if j + 1 < len(terms) else terms[j] for j in range(0, len(terms), 2)]
        return terms[0]

    comps = []
    for axis in range(3):
        comps.append(total(f[p] - f[p + 1] for p in range(1, 19, 2) if LATTICE[p][axis] == 1)
                     + 0.0)
    for axis in range(3):
        extra = [f[p] - f[p + 1] for p in range(1, 19, 2) if LATTICE[p][axis] == -1]
        if extra:
            comps[axis] = comps[axis] - total(extra)
    return total(f), comps[0], comps[1], comps[2]


def equilibrium_parts(rho, jx, jy, jz):
    inverse = 3.0 / jnp.maximum(rho, 0.5)
    v = (jx * inverse, jy * inverse, jz * inverse)
    base = 1.0 - (v[0] * v[0] + v[1] * v[1] + v[2] * v[2]) * (1.5 / 9.0)
    return v, base


def projected(v, i):
    out = None
    for comp, vel in zip(LATTICE[i], v):
        if comp == 1:
            out = vel if out is None else out + vel
        elif comp == -1:
            out = -vel if out is None else out - vel
    return out


def collide(f, omega, solid):
    rho, jx, jy, jz = moments(f)
    v, base = equilibrium_parts(rho, jx, jy, jz)
    keep = 1.0 - omega
    scale = omega * rho
    scaled = {w: scale * w for w in set(WEIGHTS)}
    post = [None] * 19
    post[0] = jnp.where(solid, f[0], keep * f[0] + scaled[WEIGHTS[0]] * base)
    for i in range(1, 19, 2):
        p = projected(v, i)
        even = base + 0.5 * (p * p)
        w = scaled[WEIGHTS[i]]
        post[i] = jnp.where(solid, f[i + 1], keep * f[i] + w * (even + p))
        post[i + 1] = jnp.where(solid, f[i], keep * f[i + 1] + w * (even - p))
    return post


def kernel(sizes, pop_hbm, omega_hbm, obstacle_hbm, total_ref, after_hbm, change_hbm,
           f_in, om, ob, post, xs, xc, ys, es, hx, hy, hz, hxy, hyz, hxz, cs, before, after, gather,
           load_sem, out_sem, send_sem, recv_sem, gsend_sem, grecv_sem):
    Z, X, Y = om.shape
    nx, ny, nz = (sizes[a] for a in AXES)
    n = nx * ny * nz
    me = tuple(lax.axis_index(a) for a in AXES)

    def device(offset):
        return {a: lax.rem(me[d] + (offset[d] % sizes[a]), sizes[a]) for d, a in enumerate(AXES)}

    loads = []
    for z in range(Z):
        loads.append(pltpu.make_async_copy(pop_hbm.at[:, z], f_in.at[:, z], load_sem.at[z]))
    loads.append(pltpu.make_async_copy(omega_hbm, om, load_sem.at[Z]))
    loads.append(pltpu.make_async_copy(obstacle_hbm, ob, load_sem.at[Z + 1]))
    for copy in loads[::-1]:
        copy.start()

    far = (nx // 2, ny // 2, nz // 2)
    covered = max(max(far), (sum(far) + 1) // 2) <= STEPS
    wrapped = lambda c: (c[0] % nx, c[1] % ny, c[2] % nz)
    everyone = [(k // (ny * nz), k // nz % ny, k % nz) for k in range(1, n)]
    greet = sorted({wrapped(c) for c in LATTICE} - {(0, 0, 0)}) if covered else everyone
    barrier = pltpu.get_barrier_semaphore()
    for offset in greet:
        pl.semaphore_signal(barrier, inc=1, device_id=device(offset), device_id_type=pl.DeviceIdType.MESH)

    lane = lax.broadcasted_iota(jnp.int32, (X, Y), 1)
    row = lax.broadcasted_iota(jnp.int32, (X, Y), 0)
    zrow = lax.broadcasted_iota(jnp.int32, (Z, Y), 0)
    zlane = lax.broadcasted_iota(jnp.int32, (Z, Y), 1)
    zsides = (1,) if nz == 2 else (1, -1)
    zside = lambda c: 0 if nz == 2 else side(c)

    def messages(s):
        out = []
        for c in (1, -1):
            d = side(c)
            out.append(((0, 0, c), post.at[s, pl.ds(9 + 5 * d, 5), Z - 1 if c == 1 else 0], hz.at[s, d]))
            out.append(((c, 0, 0), xs.at[s, d], hx.at[s, d]))
            out.append(((0, c, 0), ys.at[s, d], hy.at[s, d]))
            for b in (1, -1):
                out.append(((c, b, 0), xc.at[s, d, side(b)], hxy.at[s, d, side(b)]))
            for b in zsides:
                out.append(((0, c, b), ys.at[s, d], hyz.at[s, d, zside(b)]))
                out.append(((c, 0, b), es.at[s, d], hxz.at[s, d, zside(b)]))
        copies = [
            (offset, pltpu.make_async_remote_copy(
                src_ref=src, dst_ref=dst, send_sem=send_sem.at[s, m], recv_sem=recv_sem.at[s, m],
                device_id=device(offset), device_id_type=pl.DeviceIdType.MESH))
            for m, (offset, src, dst) in enumerate(out)
        ]
        along_x = [c for o, c in copies if o[0]]
        along_z = [c for o, c in copies if not o[0] and not o[1]]
        along_y = [c for o, c in copies if not o[0] and o[1]]
        return along_x, along_z, along_y

    def pack_x(s):
        for d in (0, 1):
            edge = X - 1 if d == 0 else 0
            for k, i in enumerate(CROSS[0][d]):
                xs[s, d, k] = post[s, SLOT[i], :, edge, :]
            for b in (1, -1):
                far_end = Y - 1 if b == 1 else 0
                line = post[s, SLOT[INDEX[(1 - 2 * d, b, 0)]], :, edge, :][:, far_end:far_end + 1]
                spots = jnp.where(zlane == zrow, jnp.broadcast_to(line, (Z, Y)), 0.0)
                xc[s, d, side(b)] = jnp.sum(spots, axis=0, keepdims=True)
            first = post[s, SLOT[INDEX[(1 - 2 * d, 0, 1)]], Z - 1, edge:edge + 1, :]
            second = post[s, SLOT[INDEX[(1 - 2 * d, 0, -1)]], 0, edge:edge + 1, :]
            es[s, d, 0] = first
            es[s, d, 1] = second

    def pack_y(s):
        for d in (0, 1):
            edge = Y - 1 if d == 0 else 0
            tile = jnp.zeros((X, Y), jnp.float32)
            for k, i in enumerate(CROSS[1][d]):
                for z in range(Z):
                    m = k * Z + z
                    moved = pltpu.roll(post[s, SLOT[i], z], (m - edge) % Y, 1)
                    tile = jnp.where(lane == m, moved, tile)
            ys[s, d] = tile

    def columns(s):
        for d in (0, 1):
            for k, i in enumerate(CROSS[0][d]):
                cx, cy, cz = LATTICE[i]
                col = hx[s, d, k]
                if cy:
                    edge = 0 if cy == 1 else Y - 1
                    spots = jnp.where(zlane == zrow, jnp.broadcast_to(hxy[s, d, side(cy)], (Z, Y)), 0.0)
                    corner = jnp.broadcast_to(jnp.sum(spots, axis=1, keepdims=True), (Z, Y))
                    col = jnp.where(zlane == edge, corner, pltpu.roll(col, cy % Y, 1))
                if cz:
                    edge = 0 if cz == 1 else Z - 1
                    r = 0 if cz == 1 else 1
                    corner = jnp.broadcast_to(hxz[s, d, zside(cz), r], (Z, Y))
                    col = jnp.where(zrow == edge, corner, pltpu.roll(col, cz % Z, 0))
                cs[s, d, k] = col

    def streamed(s, z):
        out = []
        for i in range(19):
            cx, cy, cz = LATTICE[i]
            zs = z - cz
            inside = 0 <= zs < Z
            tile = post[s, SLOT[i], zs] if inside else hz[s, side(cz), rank_in(2, i)]
            if cy:
                source = hy[s, side(cy)] if inside else hyz[s, side(cy), zside(cz)]
                m = rank_in(1, i) * Z + zs % Z
                edge = 0 if cy == 1 else Y - 1
                tile = jnp.where(lane == edge, pltpu.roll(source, (edge - m) % Y, 1), pltpu.roll(tile, cy % Y, 1))
            if cx:
                edge = 0 if cx == 1 else X - 1
                col = jnp.broadcast_to(cs[s, side(cx), rank_in(0, i), z:z + 1, :], (X, Y))
                tile = jnp.where(row == edge, col, pltpu.roll(tile, cx % X, 0))
            out.append(tile)
        return out

    sent = []
    loads[Z].wait()
    loads[Z + 1].wait()
    for s in range(STEPS):
        if s:
            columns(s - 1)
        for z in range(Z):
            if s == 0:
                loads[z].wait()
                f = [f_in[i, z] for i in range(19)]
            else:
                f = streamed(s - 1, z)
            if s == STEPS - 1:
                for c, value in enumerate(moments(f)):
                    before[c, z] = value
            new = collide(f, om[z], ob[z] == 1)
            for i in range(19):
                post[s, SLOT[i], z] = new[i]
        along_x, along_z, along_y = messages(s)
        pack_x(s)
        if s == 0:
            pl.semaphore_wait(barrier, len(greet))
        for copy in along_x + along_z:
            copy.start()
        pack_y(s)
        for copy in along_y:
            copy.start()
        copies = along_y + along_z + along_x
        for copy in copies:
            copy.wait_recv()
        sent += copies

    columns(STEPS - 1)
    sums = [jnp.zeros((X, Y), jnp.float32) for _ in range(10)]
    for z in range(Z):
        b = moments(streamed(STEPS - 1, z))
        diff = []
        for c in range(4):
            after[c, z] = b[c]
            delta = b[c] - before[c, z]
            before[c, z] = delta
            diff.append(delta)
        change_mom = diff[1] * diff[1] + diff[2] * diff[2] + diff[3] * diff[3]
        terms = (diff[0] * diff[0], change_mom, b[1], b[2], b[3], diff[1], diff[2], diff[3],
                 b[1] * b[1] + b[2] * b[2] + b[3] * b[3],
                 b[1] * diff[1] + b[2] * diff[2] + b[3] * diff[3])
        sums = [a + t for a, t in zip(sums, terms)]
    wide = lax.broadcasted_iota(jnp.int32, (1, Y), 1)
    mine = jnp.zeros((1, Y), jnp.float32)
    for k, tile in enumerate(sums):
        whole = jnp.sum(jnp.sum(tile, axis=0, keepdims=True), axis=1, keepdims=True)
        mine = jnp.where(wide == k, whole, mine)
    slot = (me[0] * ny + me[1]) * nz + me[2]
    gather[slot] = mine
    stat = []
    for k, offset in enumerate(everyone):
        stat.append(pltpu.make_async_remote_copy(
            src_ref=gather.at[slot], dst_ref=gather.at[slot], send_sem=gsend_sem.at[k], recv_sem=grecv_sem.at[k],
            device_id=device(offset), device_id_type=pl.DeviceIdType.MESH))
    for copy in stat:
        copy.start()
    out = [pltpu.make_async_copy(after, after_hbm, out_sem.at[0]),
           pltpu.make_async_copy(before, change_hbm, out_sem.at[1])]
    for copy in out:
        copy.start()
    for copy in sent:
        copy.wait_send()
    for copy in stat:
        copy.wait_recv()
    total_ref[...] = jnp.sum(gather[...], axis=0)
    for copy in stat:
        copy.wait_send()
    for copy in out:
        copy.wait()


def lift_kernel(cells, total_ref, after, before, lifted_ref, diag_ref):
    Z, X, Y = after.shape[1:]
    wide = lax.broadcasted_iota(jnp.int32, (1, Y), 1)
    total = total_ref[...]
    pick = lambda k: jnp.sum(jnp.where(wide == k, total, 0.0), axis=1, keepdims=True)
    t = [pick(k) for k in range(10)]
    change = (t[0] + t[1]) / cells
    gain = JUMP / (1.0 + LIMITER * change)
    diag = [change] + [(t[2 + c] + gain * t[5 + c]) / cells for c in range(3)]
    diag.append((t[8] + 2.0 * gain * t[9] + gain * gain * t[1]) / cells)
    for k, value in enumerate(diag):
        diag_ref[k] = value[0, 0]
    spread = jnp.broadcast_to(gain, (X, Y))
    for z in range(Z):
        rho, jx, jy, jz = (after[c, z] + spread * before[c, z] for c in range(4))
        v, base = equilibrium_parts(rho, jx, jy, jz)
        scaled = {w: rho * w for w in set(WEIGHTS)}
        lifted_ref[0, z] = scaled[WEIGHTS[0]] * base
        for i in range(1, 19, 2):
            p = projected(v, i)
            even = base + 0.5 * (p * p)
            lifted_ref[i, z] = scaled[WEIGHTS[i]] * (even + p)
            lifted_ref[i + 1, z] = scaled[WEIGHTS[i]] * (even - p)


def solution(mesh):
    sizes = {a: mesh.shape[a] for a in AXES}
    n = sizes["gx"] * sizes["gy"] * sizes["gz"]

    def per_device(populations, omega, obstacle):
        Z, X, Y = omega.shape
        S = STEPS
        nzs = 1 if sizes["gz"] == 2 else 2
        count = 10 + 4 * nzs
        f32 = lambda *shape: pltpu.VMEM(shape, jnp.float32)
        shape = lambda *dims: jax.ShapeDtypeStruct(dims, jnp.float32)
        vmem, smem = pl.BlockSpec(memory_space=pltpu.VMEM), pl.BlockSpec(memory_space=pltpu.SMEM)
        any_space = pl.BlockSpec(memory_space=pl.ANY)
        total, after, change = pl.pallas_call(
            functools.partial(kernel, sizes),
            out_shape=(shape(1, Y), shape(4, Z, X, Y), shape(4, Z, X, Y)),
            in_specs=[pl.BlockSpec(memory_space=pl.ANY)] * 3,
            out_specs=(vmem, any_space, any_space),
            scratch_shapes=[
                f32(19, Z, X, Y), f32(Z, X, Y), pltpu.VMEM((Z, X, Y), jnp.int32),
                f32(S, 19, Z, X, Y),
                f32(S, 2, 5, Z, Y), f32(S, 2, 2, 1, Y), f32(S, 2, X, Y), f32(S, 2, 2, 1, Y),
                f32(S, 2, 5, Z, Y), f32(S, 2, X, Y), f32(S, 2, 5, X, Y),
                f32(S, 2, 2, 1, Y), f32(S, 2, nzs, X, Y), f32(S, 2, nzs, 2, 1, Y),
                f32(S, 2, 5, Z, Y), f32(4, Z, X, Y), f32(4, Z, X, Y), f32(n, 1, Y),
                pltpu.SemaphoreType.DMA((Z + 2,)), pltpu.SemaphoreType.DMA((2,)),
                pltpu.SemaphoreType.DMA((S, count)), pltpu.SemaphoreType.DMA((S, count)),
                pltpu.SemaphoreType.DMA((n,)), pltpu.SemaphoreType.DMA((n,)),
            ],
            compiler_params=pltpu.CompilerParams(collective_id=0, has_side_effects=True),
        )(populations, omega, obstacle)
        return pl.pallas_call(
            functools.partial(lift_kernel, float(Z * X * Y * n)),
            out_shape=(shape(*populations.shape), shape(5)),
            in_specs=[vmem] * 3,
            out_specs=(vmem, smem),
        )(total, after, change)

    spec = P("gz", "gx", "gy")
    return jax.shard_map(
        per_device, mesh=mesh, in_specs=(P(None, *spec), spec, spec),
        out_specs=(P(None, *spec), P()), check_vma=False)
```

```python
import functools

import jax
import jax.numpy as jnp
from jax import lax
from jax.experimental import pallas as pl
from jax.experimental.pallas import tpu as pltpu
from jax.sharding import PartitionSpec as P

STEPS = 4
JUMP = 2
LIMITER = 25.0
AXES = ("gx", "gy", "gz")

LATTICE = [
    (0, 0, 0),
    (1, 0, 0), (-1, 0, 0), (0, 1, 0), (0, -1, 0), (0, 0, 1), (0, 0, -1),
    (1, 1, 0), (-1, -1, 0), (1, -1, 0), (-1, 1, 0),
    (1, 0, 1), (-1, 0, -1), (1, 0, -1), (-1, 0, 1),
    (0, 1, 1), (0, -1, -1), (0, 1, -1), (0, -1, 1),
]
WEIGHTS = [1.0 / 3.0] + [1.0 / 18.0] * 6 + [1.0 / 36.0] * 12
CROSS = [[[i for i in range(19) if LATTICE[i][axis] == sign] for sign in (1, -1)] for axis in range(3)]
ORDER = [i for i in range(19) if LATTICE[i][2] == 0] + CROSS[2][0] + CROSS[2][1]
SLOT = {i: ORDER.index(i) for i in range(19)}
INDEX = {v: i for i, v in enumerate(LATTICE)}


def side(c):
    return 0 if c == 1 else 1


def rank_in(axis, i):
    return CROSS[axis][side(LATTICE[i][axis])].index(i)


def moments(f):
    def total(terms):
        terms = list(terms)
        while len(terms) > 1:
            terms = [terms[j] + terms[j + 1] if j + 1 < len(terms) else terms[j] for j in range(0, len(terms), 2)]
        return terms[0]

    comps = []
    for axis in range(3):
        comps.append(total(f[p] - f[p + 1] for p in range(1, 19, 2) if LATTICE[p][axis] == 1)
                     + 0.0)
    for axis in range(3):
        extra = [f[p] - f[p + 1] for p in range(1, 19, 2) if LATTICE[p][axis] == -1]
        if extra:
            comps[axis] = comps[axis] - total(extra)
    return total(f), comps[0], comps[1], comps[2]


def equilibrium_parts(rho, jx, jy, jz):
    inverse = 3.0 / jnp.maximum(rho, 0.5)
    v = (jx * inverse, jy * inverse, jz * inverse)
    base = 1.0 - (v[0] * v[0] + v[1] * v[1] + v[2] * v[2]) * (1.5 / 9.0)
    return v, base


def projected(v, i):
    out = None
    for comp, vel in zip(LATTICE[i], v):
        if comp == 1:
            out = vel if out is None else out + vel
        elif comp == -1:
            out = -vel if out is None else out - vel
    return out


def collide(f, omega, solid):
    rho, jx, jy, jz = moments(f)
    v, base = equilibrium_parts(rho, jx, jy, jz)
    keep = 1.0 - omega
    scale = omega * rho
    scaled = {w: scale * w for w in set(WEIGHTS)}
    post = [None] * 19
    post[0] = jnp.where(solid, f[0], keep * f[0] + scaled[WEIGHTS[0]] * base)
    for i in range(1, 19, 2):
        p = projected(v, i)
        even = base + 0.5 * (p * p)
        w = scaled[WEIGHTS[i]]
        post[i] = jnp.where(solid, f[i + 1], keep * f[i] + w * (even + p))
        post[i + 1] = jnp.where(solid, f[i], keep * f[i + 1] + w * (even - p))
    return post


def kernel(sizes, pop_hbm, omega_hbm, obstacle_hbm, total_ref, after_hbm, change_hbm,
           f_in, om, ob, post, xs, xc, ys, es, hx, hy, hz, hxy, hyz, hxz, cs, before, after, gather,
           load_sem, out_sem, send_sem, recv_sem, gsend_sem, grecv_sem):
    Z, X, Y = om.shape
    nx, ny, nz = (sizes[a] for a in AXES)
    n = nx * ny * nz
    me = tuple(lax.axis_index(a) for a in AXES)

    def device(offset):
        return {a: lax.rem(me[d] + (offset[d] % sizes[a]), sizes[a]) for d, a in enumerate(AXES)}

    loads = []
    for z in range(Z):
        loads.append(pltpu.make_async_copy(pop_hbm.at[:, z], f_in.at[:, z], load_sem.at[z]))
    loads.append(pltpu.make_async_copy(omega_hbm, om, load_sem.at[Z]))
    loads.append(pltpu.make_async_copy(obstacle_hbm, ob, load_sem.at[Z + 1]))
    for copy in loads[::-1]:
        copy.start()

    far = (nx // 2, ny // 2, nz // 2)
    covered = max(max(far), (sum(far) + 1) // 2) <= STEPS
    wrapped = lambda c: (c[0] % nx, c[1] % ny, c[2] % nz)
    everyone = [(k // (ny * nz), k // nz % ny, k % nz) for k in range(1, n)]
    greet = sorted({wrapped(c) for c in LATTICE} - {(0, 0, 0)}) if covered else everyone
    barrier = pltpu.get_barrier_semaphore()
    for offset in greet:
        pl.semaphore_signal(barrier, inc=1, device_id=device(offset), device_id_type=pl.DeviceIdType.MESH)

    lane = lax.broadcasted_iota(jnp.int32, (X, Y), 1)
    row = lax.broadcasted_iota(jnp.int32, (X, Y), 0)
    zrow = lax.broadcasted_iota(jnp.int32, (Z, Y), 0)
    zlane = lax.broadcasted_iota(jnp.int32, (Z, Y), 1)
    zsides = (1,) if nz == 2 else (1, -1)
    zside = lambda c: 0 if nz == 2 else side(c)

    def messages(s):
        out = []
        for c in (1, -1):
            d = side(c)
            out.append(((0, 0, c), post.at[s, pl.ds(9 + 5 * d, 5), Z - 1 if c == 1 else 0], hz.at[s, d]))
            out.append(((c, 0, 0), xs.at[s, d], hx.at[s, d]))
            out.append(((0, c, 0), ys.at[s, d], hy.at[s, d]))
            for b in (1, -1):
                out.append(((c, b, 0), xc.at[s, d, side(b)], hxy.at[s, d, side(b)]))
            for b in zsides:
                out.append(((0, c, b), ys.at[s, d], hyz.at[s, d, zside(b)]))
                out.append(((c, 0, b), es.at[s, d], hxz.at[s, d, zside(b)]))
        copies = [
            (offset, pltpu.make_async_remote_copy(
                src_ref=src, dst_ref=dst, send_sem=send_sem.at[s, m], recv_sem=recv_sem.at[s, m],
                device_id=device(offset), device_id_type=pl.DeviceIdType.MESH))
            for m, (offset, src, dst) in enumerate(out)
        ]
        along_x = [c for o, c in copies if o[0]]
        along_z = [c for o, c in copies if not o[0] and not o[1]]
        along_y = [c for o, c in copies if not o[0] and o[1]]
        return along_x, along_z, along_y

    def pack_x(s):
        for d in (0, 1):
            edge = X - 1 if d == 0 else 0
            for k, i in enumerate(CROSS[0][d]):
                xs[s, d, k] = post[s, SLOT[i], :, edge, :]
            for b in (1, -1):
                far_end = Y - 1 if b == 1 else 0
                line = post[s, SLOT[INDEX[(1 - 2 * d, b, 0)]], :, edge, :][:, far_end:far_end + 1]
                spots = jnp.where(zlane == zrow, jnp.broadcast_to(line, (Z, Y)), 0.0)
                xc[s, d, side(b)] = jnp.sum(spots, axis=0, keepdims=True)
            first = post[s, SLOT[INDEX[(1 - 2 * d, 0, 1)]], Z - 1, edge:edge + 1, :]
            second = post[s, SLOT[INDEX[(1 - 2 * d, 0, -1)]], 0, edge:edge + 1, :]
            es[s, d, 0] = first
            es[s, d, 1] = second

    def pack_y(s):
        for d in (0, 1):
            edge = Y - 1 if d == 0 else 0
            tile = jnp.zeros((X, Y), jnp.float32)
            for k, i in enumerate(CROSS[1][d]):
                for z in range(Z):
                    m = k * Z + z
                    moved = pltpu.roll(post[s, SLOT[i], z], (m - edge) % Y, 1)
                    tile = jnp.where(lane == m, moved, tile)
            ys[s, d] = tile

    def columns(s):
        for d in (0, 1):
            for k, i in enumerate(CROSS[0][d]):
                cx, cy, cz = LATTICE[i]
                col = hx[s, d, k]
                if cy:
                    edge = 0 if cy == 1 else Y - 1
                    spots = jnp.where(zlane == zrow, jnp.broadcast_to(hxy[s, d, side(cy)], (Z, Y)), 0.0)
                    corner = jnp.broadcast_to(jnp.sum(spots, axis=1, keepdims=True), (Z, Y))
                    col = jnp.where(zlane == edge, corner, pltpu.roll(col, cy % Y, 1))
                if cz:
                    edge = 0 if cz == 1 else Z - 1
                    r = 0 if cz == 1 else 1
                    corner = jnp.broadcast_to(hxz[s, d, zside(cz), r], (Z, Y))
                    col = jnp.where(zrow == edge, corner, pltpu.roll(col, cz % Z, 0))
                cs[s, d, k] = col

    def streamed(s, z):
        out = []
        for i in range(19):
            cx, cy, cz = LATTICE[i]
            zs = z - cz
            inside = 0 <= zs < Z
            tile = post[s, SLOT[i], zs] if inside else hz[s, side(cz), rank_in(2, i)]
            if cy:
                source = hy[s, side(cy)] if inside else hyz[s, side(cy), zside(cz)]
                m = rank_in(1, i) * Z + zs % Z
                edge = 0 if cy == 1 else Y - 1
                tile = jnp.where(lane == edge, pltpu.roll(source, (edge - m) % Y, 1), pltpu.roll(tile, cy % Y, 1))
            if cx:
                edge = 0 if cx == 1 else X - 1
                col = jnp.broadcast_to(cs[s, side(cx), rank_in(0, i), z:z + 1, :], (X, Y))
                tile = jnp.where(row == edge, col, pltpu.roll(tile, cx % X, 0))
            out.append(tile)
        return out

    sent = []
    loads[Z].wait()
    loads[Z + 1].wait()
    for s in range(STEPS):
        if s:
            columns(s - 1)
        for z in range(Z):
            if s == 0:
                loads[z].wait()
                f = [f_in[i, z] for i in range(19)]
            else:
                f = streamed(s - 1, z)
            if s == STEPS - 1:
                for c, value in enumerate(moments(f)):
                    before[c, z] = value
            new = collide(f, om[z], ob[z] == 1)
            for i in range(19):
                post[s, SLOT[i], z] = new[i]
        along_x, along_z, along_y = messages(s)
        if s == 0:
            pl.semaphore_wait(barrier, len(greet))
        for copy in along_z:
            copy.start()
        pack_x(s)
        for copy in along_x:
            copy.start()
        pack_y(s)
        for copy in along_y:
            copy.start()
        copies = along_y + along_z + along_x
        for copy in copies:
            copy.wait_recv()
        sent += copies

    columns(STEPS - 1)
    sums = [jnp.zeros((X, Y), jnp.float32) for _ in range(10)]
    for z in range(Z):
        b = moments(streamed(STEPS - 1, z))
        diff = []
        for c in range(4):
            after[c, z] = b[c]
            delta = b[c] - before[c, z]
            before[c, z] = delta
            diff.append(delta)
        change_mom = diff[1] * diff[1] + diff[2] * diff[2] + diff[3] * diff[3]
        terms = (diff[0] * diff[0], change_mom, b[1], b[2], b[3], diff[1], diff[2], diff[3],
                 b[1] * b[1] + b[2] * b[2] + b[3] * b[3],
                 b[1] * diff[1] + b[2] * diff[2] + b[3] * diff[3])
        sums = [a + t for a, t in zip(sums, terms)]
    wide = lax.broadcasted_iota(jnp.int32, (1, Y), 1)
    mine = jnp.zeros((1, Y), jnp.float32)
    for k, tile in enumerate(sums):
        whole = jnp.sum(jnp.sum(tile, axis=0, keepdims=True), axis=1, keepdims=True)
        mine = jnp.where(wide == k, whole, mine)
    slot = (me[0] * ny + me[1]) * nz + me[2]
    gather[slot] = mine
    stat = []
    hops = lambda o: sum(min(c, m - c) for c, m in zip(o, (nx, ny, nz)))
    for k, offset in enumerate(sorted(everyone, key=lambda o: -hops(o))):
        stat.append(pltpu.make_async_remote_copy(
            src_ref=gather.at[slot], dst_ref=gather.at[slot], send_sem=gsend_sem.at[k], recv_sem=grecv_sem.at[k],
            device_id=device(offset), device_id_type=pl.DeviceIdType.MESH))
    for copy in stat:
        copy.start()
    out = [pltpu.make_async_copy(after, after_hbm, out_sem.at[0]),
           pltpu.make_async_copy(before, change_hbm, out_sem.at[1])]
    for copy in out:
        copy.start()
    for copy in sent:
        copy.wait_send()
    for copy in stat:
        copy.wait_recv()
    total_ref[...] = jnp.sum(gather[...], axis=0)
    for copy in stat:
        copy.wait_send()
    for copy in out:
        copy.wait()


def lift_kernel(cells, total_ref, after, before, lifted_ref, diag_ref):
    Z, X, Y = after.shape[1:]
    wide = lax.broadcasted_iota(jnp.int32, (1, Y), 1)
    total = total_ref[...]
    pick = lambda k: jnp.sum(jnp.where(wide == k, total, 0.0), axis=1, keepdims=True)
    t = [pick(k) for k in range(10)]
    change = (t[0] + t[1]) / cells
    gain = JUMP / (1.0 + LIMITER * change)
    diag = [change] + [(t[2 + c] + gain * t[5 + c]) / cells for c in range(3)]
    diag.append((t[8] + 2.0 * gain * t[9] + gain * gain * t[1]) / cells)
    for k, value in enumerate(diag):
        diag_ref[k] = value[0, 0]
    spread = jnp.broadcast_to(gain, (X, Y))
    for z in range(Z):
        rho, jx, jy, jz = (after[c, z] + spread * before[c, z] for c in range(4))
        v, base = equilibrium_parts(rho, jx, jy, jz)
        scaled = {w: rho * w for w in set(WEIGHTS)}
        lifted_ref[0, z] = scaled[WEIGHTS[0]] * base
        for i in range(1, 19, 2):
            p = projected(v, i)
            even = base + 0.5 * (p * p)
            lifted_ref[i, z] = scaled[WEIGHTS[i]] * (even + p)
            lifted_ref[i + 1, z] = scaled[WEIGHTS[i]] * (even - p)


def solution(mesh):
    sizes = {a: mesh.shape[a] for a in AXES}
    n = sizes["gx"] * sizes["gy"] * sizes["gz"]

    def per_device(populations, omega, obstacle):
        Z, X, Y = omega.shape
        S = STEPS
        nzs = 1 if sizes["gz"] == 2 else 2
        count = 10 + 4 * nzs
        f32 = lambda *shape: pltpu.VMEM(shape, jnp.float32)
        shape = lambda *dims: jax.ShapeDtypeStruct(dims, jnp.float32)
        vmem, smem = pl.BlockSpec(memory_space=pltpu.VMEM), pl.BlockSpec(memory_space=pltpu.SMEM)
        any_space = pl.BlockSpec(memory_space=pl.ANY)
        total, after, change = pl.pallas_call(
            functools.partial(kernel, sizes),
            out_shape=(shape(1, Y), shape(4, Z, X, Y), shape(4, Z, X, Y)),
            in_specs=[pl.BlockSpec(memory_space=pl.ANY)] * 3,
            out_specs=(vmem, any_space, any_space),
            scratch_shapes=[
                f32(19, Z, X, Y), f32(Z, X, Y), pltpu.VMEM((Z, X, Y), jnp.int32),
                f32(S, 19, Z, X, Y),
                f32(S, 2, 5, Z, Y), f32(S, 2, 2, 1, Y), f32(S, 2, X, Y), f32(S, 2, 2, 1, Y),
                f32(S, 2, 5, Z, Y), f32(S, 2, X, Y), f32(S, 2, 5, X, Y),
                f32(S, 2, 2, 1, Y), f32(S, 2, nzs, X, Y), f32(S, 2, nzs, 2, 1, Y),
                f32(S, 2, 5, Z, Y), f32(4, Z, X, Y), f32(4, Z, X, Y), f32(n, 1, Y),
                pltpu.SemaphoreType.DMA((Z + 2,)), pltpu.SemaphoreType.DMA((2,)),
                pltpu.SemaphoreType.DMA((S, count)), pltpu.SemaphoreType.DMA((S, count)),
                pltpu.SemaphoreType.DMA((n,)), pltpu.SemaphoreType.DMA((n,)),
            ],
            compiler_params=pltpu.CompilerParams(collective_id=0, has_side_effects=True),
        )(populations, omega, obstacle)
        return pl.pallas_call(
            functools.partial(lift_kernel, float(Z * X * Y * n)),
            out_shape=(shape(*populations.shape), shape(5)),
            in_specs=[vmem] * 3,
            out_specs=(vmem, smem),
        )(total, after, change)

    spec = P("gz", "gx", "gy")
    return jax.shard_map(
        per_device, mesh=mesh, in_specs=(P(None, *spec), spec, spec),
        out_specs=(P(None, *spec), P()), check_vma=False)
```
